32 devices in a mesh: grp: 4 (over z), head: 8 (over y, x, core).
Axes of the slice: x: 2, y: 2, z: 4, core: 2. Of those that a mesh axis runs over, the one named last changes fastest.
Arguments:
- inputs: bfloat16 [4, 64, 4096], P(None, 'grp', 'head'), parts along dimension 1, may hold values from -6 to 6
- gains: float32 [2, 4096], replicated, may hold values from 0.5 to 1.5
- decays: float32 [2, 32], P(None, 'head'), may hold values from 0.7 to 0.999
- w_qkv: bfloat16 [2, 4096, 3, 32, 128], P(None, None, None, 'head'), may hold values from -0.09375 to 0.09375
- w_out: bfloat16 [2, 32, 128, 4096], P(None, 'head'), may hold values from -0.125 to 0.125
- s_state: float32 [2, 64, 32, 128, 128], P(None, 'grp', 'head'), parts along dimension 1, may hold values from -0.5 to 0.5
- r_state: float32 [2, 64, 32, 128, 128], P(None, 'grp', 'head'), parts along dimension 1, as said below
Outputs:
- stream_out: float32 [4, 64, 4096], P(None, 'grp', 'head'), parts along dimension 1
- s_final: float32 [2, 64, 32, 128, 128], P(None, 'grp', 'head'), parts along dimension 1
- r_final: float32 [2, 64, 32, 128, 128], P(None, 'grp', 'head'), parts along dimension 1
The draws below stay inside these ranges and needn't reach their ends.
There are 4 independent parts, one for each index of `grp`. The reference program is written for one: setup_inputs(seed, part) draws one part's arguments, and reference() takes and returns one part's arrays. A program takes and returns all parts, laid end to end along the dimension named above; an argument that names none is the same for every part. Nothing has to cross between parts.
Inputs may be any that keep to these rules, and one draw needn't show every extreme that they name: `r_state`: each matrix is symmetric positive definite with eigenvalues of 0.5 or more and of order one.
All inputs are finite; a program needn't handle non-finite values.
Results may differ from the reference program's by a relative error of at most 0.02.
Values may be sent and summed in bfloat16 or wider, within the bound.
A program may use at most 192 MiB of HBM per device.

```python
import math
import jax
import jax.numpy as jnp
from jax import lax

D = 4096
H = 32
HD = 128
B = 16
TOKS = 4
LAYERS = 2


def draw_r_state(key, part):
    factor = jax.random.normal(key, (LAYERS, B, H, HD, HD), jnp.float32)
    product = jnp.einsum('lbhij,lbhkj->lbhik', factor, factor, precision=lax.Precision.HIGHEST)
    return 0.5 * jnp.eye(HD, dtype=jnp.float32) + product / HD


def spiked(values, key, source, target, parts, factor):
    owner, partner = [(jnp.arange(values.shape[dim]) // (values.shape[dim] // parts)).reshape([-1 if axis == dim else 1 for axis in range(values.ndim)]) for dim in (source, target)]
    chosen = jax.random.permutation(key, parts)[partner]
    strong = (owner == chosen) | (owner == (partner + parts // 2) % parts)
    return jnp.where(strong, factor * values, values)


def shard_levels(own_key, extent, pieces, smallest, largest):
    level, own = 1.0, jax.random.fold_in(own_key, 6)
    for axis_at, blocks in pieces:
        draws = jnp.exp(jax.random.uniform(jax.random.fold_in(own, axis_at), (blocks,), jnp.float32, smallest / len(pieces), largest / len(pieces)))
        level = level * jnp.repeat(draws, extent[axis_at] // blocks).reshape([-1 if axis == axis_at else 1 for axis in range(len(extent))])
    return level


def scatter_about(rng, extent, scale, reach, shards=(), kind=jnp.bfloat16):
    values = scale * jax.random.normal(rng, extent, jnp.float32)
    if shards:
        values = values * shard_levels(rng, extent, shards, -0.22, 0.18)
    return jnp.clip(values, -reach, reach).astype(kind)


def noise_with(key, dims, spread, reach, shards, heavy, kind=jnp.bfloat16):
    array = spread * jax.random.normal(key, dims, jnp.float32)
    if shards:
        array = array * shard_levels(key, dims, shards, -0.22, 0.18)
    return jnp.clip(spiked(array, jax.random.fold_in(key, 3), *heavy), -reach, reach).astype(kind)


def setup_inputs(seed: int = 0, part: int = 0) -> dict:
    splits = jax.random.split(jax.random.key(seed), 8)
    part_splits = jax.random.split(jax.random.fold_in(splits[7], part), 8)
    return {
        "inputs": scatter_about(part_splits[0], (TOKS, B, D), 1.0, 6.0, ((2, 8),)),
        "gains": jnp.clip(1.0 + 0.1 * jax.random.normal(splits[1], (LAYERS, D), jnp.float32), 0.5, 1.5),
        "decays": jnp.clip(jnp.exp(math.log(0.999) - 0.35567447 * jax.random.uniform(splits[2], (LAYERS, H), jnp.float32) ** shard_levels(splits[2], (LAYERS, H), ((1, 8),), -0.2, 0.2)), 0.7, 0.999),
        "w_qkv": scatter_about(splits[3], (LAYERS, D, 3, H, HD), D ** -0.5, 0.09375, ((3, 8),)),
        "w_out": noise_with(splits[4], (LAYERS, H, HD, D), (H * HD) ** -0.5, 0.125, ((1, 8),), (1, 3, 8, 2.0)),
        "s_state": scatter_about(part_splits[5], (LAYERS, B, H, HD, HD), HD ** -0.5, 0.5, ((2, 8),), jnp.float32),
        "r_state": draw_r_state(jax.random.fold_in(jax.random.fold_in(splits[7], part), 71), part),
    }


EPSILON = 1e-05
PRECISE = lax.Precision.HIGHEST

def rescale(vector):
    return vector * lax.rsqrt(lax.optimization_barrier(jnp.mean(vector * vector, axis=-1, keepdims=True)) + EPSILON)

def mesa_step(query_vec, key_vec, value_vec, decay, states, inverse):
    applied = jnp.einsum('bhij,bhj->bhi', inverse, key_vec, precision=PRECISE)
    denominator = decay[None, :] + lax.optimization_barrier(jnp.sum(key_vec * applied, axis=-1))
    inverse = (inverse - applied[..., :, None] * applied[..., None, :] / denominator[..., None, None]) / decay[None, :, None, None]
    states = decay[None, :, None, None] * states + value_vec[..., :, None] * key_vec[..., None, :]
    weighted = jnp.einsum('bhij,bhj->bhi', inverse, query_vec, precision=PRECISE)
    output = jnp.einsum('bhij,bhj->bhi', states, weighted, precision=PRECISE)
    return (output, states, inverse)

def reference(inputs, gains, decays, w_qkv, w_out, s_state, r_state):
    stream = inputs.astype(jnp.float32)
    states = [s_state[index] for index in range(LAYERS)]
    inverses = [r_state[index] for index in range(LAYERS)]
    results = []
    for position in range(TOKS):
        current = stream[position]
        for layer_id in range(LAYERS):
            normed = (rescale(current) * gains[layer_id]).astype(jnp.bfloat16)
            projected = jnp.dot(normed, w_qkv[layer_id].reshape(D, 3 * H * HD), preferred_element_type=jnp.float32).reshape(B, 3, H, HD)
            query_vec = rescale(projected[:, 0])
            key_vec = rescale(projected[:, 1]) * HD ** (-0.5)
            value_vec = projected[:, 2]
            output, states[layer_id], inverses[layer_id] = mesa_step(query_vec, key_vec, value_vec, decays[layer_id], states[layer_id], inverses[layer_id])
            mixed = jnp.dot(output.astype(jnp.bfloat16).reshape(B, H * HD), w_out[layer_id].reshape(H * HD, D), preferred_element_type=jnp.float32)
            current = current + mixed
        results.append(current)
    return (jnp.stack(results), jnp.stack(states), jnp.stack(inverses))
```

```python
import functools

import jax
import jax.numpy as jnp
from jax import lax
from jax.experimental import pallas as pl
from jax.experimental.pallas import tpu as pltpu
from jax.sharding import PartitionSpec as P

EPSILON = 1e-05
PIECES = 4
PARTS = 1
F32 = jnp.float32
BF16 = jnp.bfloat16
MESH = pl.DeviceIdType.MESH


def front_kernel(
    n, tokens, batch, heads, layers, parts,
    x_hbm, gains_hbm, dec_hbm, w_hbm, wo_hbm, s_hbm, r_hbm,
    y_ref, sv, rv,
    xin, gains_ref, dec_ref, w, wo, spread, xg, lhs, acc, squares, near, far, pair, recv, mine, cur,
    kq, pz, os, oo, left_ref, right_ref,
    misc_sem, w_sem, wo_sem, state_sem, ag_send, ag_recv, sib_send, sib_recv, rs_send, rs_recv,
):
    me = lax.axis_index("head")
    side = lax.rem(me, 2)
    chip = me // 2
    chips = n // 2
    sibling = me + 1 - 2 * side
    hd = kq.shape[-1]
    width = gains_ref.shape[1]
    shard = xin.shape[2]
    span = batch // parts
    rows = tokens * span
    mixed = 3 * heads
    pack = lhs.shape[1] // rows
    groups = mixed // pack
    piece = width // PIECES

    def w_copies(layer):
        out = []
        for c in range(PIECES):
            at = pl.ds(c * piece, piece)
            if pack == 1:
                out.append(
                    pltpu.make_async_copy(
                        w_hbm.at[layer, at], w.at[layer, at], w_sem.at[layer, c]
                    )
                )
                continue
            octs = pl.ds(c * piece // 8, piece // 8)
            for s in range(8):
                out.append(
                    pltpu.make_async_copy(
                        w_hbm.at[layer, octs, s],
                        w.at[layer, octs, :, pl.ds(s * pack, pack)],
                        w_sem.at[layer, c],
                    )
                )
        return out

    def w_wait(layer):
        for c in range(PIECES):
            at = pl.ds(c * piece // (8 if pack > 1 else 1), piece // (8 if pack > 1 else 1))
            pltpu.make_async_copy(w.at[layer, at], w.at[layer, at], w_sem.at[layer, c]).wait()

    def wo_copy(layer):
        return pltpu.make_async_copy(wo_hbm.at[layer], wo.at[layer], wo_sem.at[layer])

    def state_copy(which, layer, part):
        src, dst = ((r_hbm, rv), (s_hbm, sv))[which]
        at = pl.ds(part * span, span)
        return pltpu.make_async_copy(
            src.at[layer, at], dst.at[layer, at], state_sem.at[which, layer, part]
        )

    started = []

    def send(src, dst, out_sem, in_sem, peer):
        copy = pltpu.make_async_remote_copy(
            src_ref=src,
            dst_ref=dst,
            send_sem=out_sem,
            recv_sem=in_sem,
            device_id={"head": peer},
            device_id_type=MESH,
        )
        copy.start()
        started.append(copy)

    def arrive(buf, sem):
        pltpu.make_async_copy(buf, buf, sem).wait()

    def peer(k):
        return lax.rem(me + 2 * k, n)

    def block_at(k, other):
        at = 2 * lax.rem(chip - k + chips, chips)
        return at + (1 - side if other else side)

    misc = (
        pltpu.make_async_copy(x_hbm, xin, misc_sem.at[0]),
        pltpu.make_async_copy(gains_hbm, gains_ref, misc_sem.at[1]),
        pltpu.make_async_copy(dec_hbm, dec_ref, misc_sem.at[2]),
    )
    for copy in misc:
        copy.start()
    barrier = pltpu.get_barrier_semaphore()
    for k in range(1, chips):
        pl.semaphore_signal(barrier, inc=1, device_id={"head": peer(k)}, device_id_type=MESH)
    pl.semaphore_signal(barrier, inc=1, device_id={"head": sibling}, device_id_type=MESH)
    for copy in w_copies(0):
        copy.start()
    for part in range(parts):
        state_copy(0, 0, part).start()
    if pack > 1:
        row = lax.broadcasted_iota(jnp.int32, spread.shape, 0)
        col = lax.broadcasted_iota(jnp.int32, spread.shape, 1)
        half = spread.shape[1] // 2
        hit = jnp.where(col < half, col - 2 * row, col - half - 2 * row - 1)
        spread[...] = jnp.where(hit == 0, 1.0, 0.0).astype(BF16)
    misc[0].wait()
    whole = [xin[t].astype(F32) for t in range(tokens)]
    for part in range(parts):
        piece_x = jnp.concatenate([v[part * span : (part + 1) * span] for v in whole], axis=0)
        cur[part] = piece_x
        xg[0, part, 0, 0] = piece_x.astype(BF16)
    pl.semaphore_wait(barrier, chips)

    def gather_start(layer, part):
        own = xg.at[layer, part, 0, 0]
        for k in range(1, chips):
            send(
                own, xg.at[layer, part, k, 0],
                ag_send.at[layer, part, 0, k], ag_recv.at[layer, part, 0, k], peer(k),
            )
        send(
            own, xg.at[layer, part, 0, 1],
            ag_send.at[layer, part, 0, 0], ag_recv.at[layer, part, 1, 0], sibling,
        )

    def forward(layer, part):
        total = expand(layer, part, 0, 0)
        arrive(xg.at[layer, part, 0, 1], ag_recv.at[layer, part, 1, 0])
        total = total + expand(layer, part, 0, 1)
        for k in range(1, chips):
            arrive(xg.at[layer, part, k, 0], ag_recv.at[layer, part, 0, k])
            send(
                xg.at[layer, part, k, 0], xg.at[layer, part, k, 1],
                ag_send.at[layer, part, 1, k], ag_recv.at[layer, part, 1, k], sibling,
            )
        for k in range(1, chips):
            total = total + expand(layer, part, k, 0)
        squares[part] = total

    def expand(layer, part, k, other):
        i = block_at(k, other)
        block = xg[layer, part, k, other].astype(F32)
        gain = gains_ref[layer : layer + 1, pl.ds(pl.multiple_of(i * shard, shard), shard)]
        square = block * block
        total = square[:, :128]
        for at in range(128, shard, 128):
            total = total + square[:, at : at + 128]
        scaled = (block * gain).astype(BF16)
        slot = 2 * k + other
        if pack == 1:
            lhs[slot] = scaled
            return total
        wide = spread.shape[1] // 2
        stack = jnp.concatenate(
            [scaled[:, at : at + 128] for at in range(0, shard, 128)], axis=0
        )
        out = jnp.dot(stack, spread[...], preferred_element_type=F32).astype(BF16)
        for s in range(shard // 128):
            for p in range(pack):
                lhs[slot, p * rows : (p + 1) * rows, s * wide : (s + 1) * wide] = out[
                    s * rows : (s + 1) * rows, p * wide : (p + 1) * wide
                ]
        return total

    def multiply(layer, part, slots, first):
        for g in range(0, groups, 2):
            many = min(2, groups - g)
            total = None
            for k, other in slots:
                i = block_at(k, other)
                if pack == 1:
                    at = pl.ds(pl.multiple_of(i * shard, shard), shard)
                    weights = w[layer, at, g * hd : (g + many) * hd]
                else:
                    at = pl.ds(i * (shard // 8), shard // 8)
                    weights = jnp.concatenate(
                        [
                            w[layer, at, g + j].reshape(pack * shard, hd)
                            for j in range(many)
                        ],
                        axis=1,
                    )
                term = jnp.dot(lhs[2 * k + other], weights, preferred_element_type=F32)
                total = term if total is None else total + term
            cols = slice(g * hd, (g + many) * hd)
            acc[part, :, cols] = total if first else acc[part, :, cols] + total

    def project_near(layer, part):
        slots = [(k, 0) for k in range(chips)] + [(0, 1)]
        multiply(layer, part, slots, True)

    def project_far(layer, part):
        slots = [(k, 1) for k in range(1, chips)]
        total = squares[part]
        for k, other in slots:
            arrive(xg.at[layer, part, k, 1], ag_recv.at[layer, part, 1, k])
        for k, other in slots:
            total = total + expand(layer, part, k, other)
        multiply(layer, part, slots, False)
        return lax.rsqrt(jnp.sum(total, axis=-1, keepdims=True) / width + EPSILON)

    def norm(v):
        return v * lax.rsqrt(jnp.mean(v * v, axis=-1, keepdims=True) + EPSILON)

    def dots(a, b):
        return jnp.sum(a * b, axis=-1, keepdims=True)

    def tok(t):
        return slice(t * span, (t + 1) * span)

    def per_pair(fn):
        step = 4 if span % 4 == 0 else 1

        def body(i, carry):
            for j in range(step):
                b = i * step + j
                for h in range(heads):
                    fn(b, h)
            return carry

        lax.fori_loop(0, span // step, body, 0)

    def mesa(layer, part, factor):
        base = part * span

        def projected(j, h):
            at = j * heads + h
            p, g = at % pack, at // pack
            return acc[part, p * rows : (p + 1) * rows, g * hd : (g + 1) * hd] * factor

        for h in range(heads):
            kq[h, rows:, :] = norm(projected(0, h))
            kq[h, :rows, :] = norm(projected(1, h)) * hd ** (-0.5)
            left_ref[layer, part, h, rows:, :] = projected(2, h)
        state_copy(0, layer, part).wait()

        def first(b, h):
            both = kq[h, pl.ds(b, 2 * tokens, stride=span), :].astype(BF16)
            pz[h, pl.ds(b, 2 * tokens, stride=span), :] = jnp.dot(
                both, rv[layer, base + b, h].astype(BF16), preferred_element_type=F32
            )

        per_pair(first)
        for h in range(heads):
            g = jnp.full((span, 1), dec_ref[layer, h], F32)
            ginv = 1.0 / g
            ks = [kq[h, tok(t), :] for t in range(tokens)]
            qs = [kq[h, tok(tokens + t), :] for t in range(tokens)]
            ps = [pz[h, tok(t), :] for t in range(tokens)]
            zs = [pz[h, tok(tokens + t), :] for t in range(tokens)]
            back = [None] * (tokens + 1)
            front = [None] * (tokens + 1)
            back[0] = front[0] = jnp.ones_like(g)
            for t in range(tokens):
                back[t + 1] = back[t] * ginv
                front[t + 1] = front[t] * g
            for t in range(tokens):
                u = ps[t]
                inv = 1.0 / (g + dots(ks[t], u))
                for s in range(t + 1, tokens):
                    ps[s] = (ps[s] - u * (dots(u, ks[s]) * inv)) * ginv
                for s in range(t, tokens):
                    zs[s] = (zs[s] - u * (dots(u, qs[s]) * inv)) * ginv
                left_ref[layer, part, h, tok(t), :] = u
                right_ref[layer, part, h, tok(t), :] = u * (-inv * back[tokens - t])
                right_ref[layer, part, h, tok(tokens + t), :] = ks[t] * front[tokens - 1 - t]
                pz[h, tok(t), :] = zs[t]
        state_copy(1, layer, part).wait()

        def second(b, h):
            both = pz[h, pl.ds(b, 2 * tokens, stride=span), :].astype(BF16)
            os[h, pl.ds(b, 2 * tokens, stride=span), :] = lax.dot_general(
                both, sv[layer, base + b, h].astype(BF16), (((1,), (1,)), ((), ())),
                preferred_element_type=F32,
            )

        per_pair(second)
        for h in range(heads):
            g = jnp.full((span, 1), dec_ref[layer, h], F32)
            front = [jnp.ones_like(g)]
            for t in range(tokens):
                front.append(front[-1] * g)
            outs = []
            for t in range(tokens):
                z = pz[h, tok(t), :]
                out = os[h, tok(t), :] * front[t + 1]
                for s in range(t + 1):
                    v = left_ref[layer, part, h, tok(tokens + s), :]
                    out = out + v * (dots(kq[h, tok(s), :], z) * front[t - s])
                outs.append(out)
            oo[part, :, h * hd : (h + 1) * hd] = jnp.concatenate(outs, axis=0).astype(BF16)

    def update(layer, part):
        base = part * span
        upper = lax.broadcasted_iota(jnp.int32, (2 * tokens, hd), 0) < tokens
        scales = []
        for h in range(heads):
            g = jnp.full((1, hd), dec_ref[layer, h], F32)
            power = g
            for _ in range(tokens - 1):
                power = power * g
            scales.append((power, 1.0 / power))

        def change_of(b, h):
            at = pl.ds(b, 2 * tokens, stride=span)
            left = left_ref[layer, part, h, at, :]
            right = right_ref[layer, part, h, at, :]
            zero = jnp.zeros_like(right)
            both = jnp.concatenate(
                [jnp.where(upper, right, zero), jnp.where(upper, zero, right)], axis=1
            ).astype(BF16)
            change = jnp.dot(left.T.astype(BF16), both, preferred_element_type=F32)
            rv[layer, base + b, h] = rv[layer, base + b, h] * scales[h][1] + change[:, :hd]
            sv[layer, base + b, h] = sv[layer, base + b, h] * scales[h][0] + change[:, hd:]

        per_pair(change_of)

    def mix(layer, part):
        def product(k, other):
            i = 2 * lax.rem(chip + k, chips) + (1 - side if other else side)
            col = pl.ds(pl.multiple_of(i * shard, shard), shard)
            return jnp.dot(oo[part], wo[layer, :, col], preferred_element_type=F32)

        order = list(range(1, chips)) + [0]
        for k in order:
            near[layer, part, k] = product(k, 1).astype(BF16)
        for k in order:
            send(
                near.at[layer, part, k], far.at[layer, part, k],
                sib_send.at[layer, part, k], sib_recv.at[layer, part, k], sibling,
            )
        for k in order:
            mine[part, k] = product(k, 0)

    def scatter(layer, part):
        for k in range(1, chips):
            arrive(far.at[layer, part, k], sib_recv.at[layer, part, k])
            pair[layer, part, k] = (
                mine[part, k] + far[layer, part, k].astype(F32)
            ).astype(BF16)
            send(
                pair.at[layer, part, k], recv.at[layer, part, k],
                rs_send.at[layer, part, k], rs_recv.at[layer, part, k], peer(k),
            )

    def collect(layer, part):
        arrive(far.at[layer, part, 0], sib_recv.at[layer, part, 0])
        total = cur[part] + mine[part, 0] + far[layer, part, 0].astype(F32)
        for k in range(1, chips):
            arrive(recv.at[layer, part, k], rs_recv.at[layer, part, k])
            total = total + recv[layer, part, k].astype(F32)
        cur[part] = total
        if layer + 1 < layers:
            xg[layer + 1, part, 0, 0] = total.astype(BF16)
            gather_start(layer + 1, part)
        else:
            for t in range(tokens):
                y_ref[t, part * span : (part + 1) * span, :] = total[t * span : (t + 1) * span]

    every = range(parts)
    for part in every:
        gather_start(0, part)
    for copy in misc[1:]:
        copy.wait()
    for layer in range(layers):
        for part in every:
            if layer > 0 and part > 0:
                collect(layer - 1, part)
            forward(layer, part)
            if part == 0:
                w_wait(layer)
                if layer == 0:
                    for p in every:
                        state_copy(1, 0, p).start()
                    wo_copy(0).start()
            project_near(layer, part)
            if part > 0:
                scatter(layer, part - 1)
            if part == 0 and layer + 1 < layers:
                for copy in w_copies(layer + 1):
                    copy.start()
            factor = project_far(layer, part)
            mesa(layer, part, factor)
            if part == 0:
                wo_copy(layer).wait()
            mix(layer, part)
            if part == 0 and layer + 1 < layers:
                for which in range(2):
                    for p in every:
                        state_copy(which, layer + 1, p).start()
                wo_copy(layer + 1).start()
        scatter(layer, parts - 1)
        if layer + 1 < layers:
            collect(layer, 0)
            for part in every:
                update(layer, part)
        else:
            for part in every:
                if part + 1 < parts:
                    collect(layer, part)
                update(layer, part)
            collect(layer, parts - 1)
    for copy in started:
        copy.wait_send()


def back_kernel(y_vmem, s_vmem, r_vmem, y_hbm, s_hbm, r_hbm, sems):
    copies = [pltpu.make_async_copy(y_vmem, y_hbm, sems.at[2, 0, 0])]
    layers, count = s_vmem.shape[:2]
    cut = count // sems.shape[2]
    for layer in range(layers):
        for c in range(sems.shape[2]):
            at = pl.ds(c * cut, cut)
            copies.append(
                pltpu.make_async_copy(
                    s_vmem.at[layer, at], s_hbm.at[layer, at], sems.at[0, layer, c]
                )
            )
            copies.append(
                pltpu.make_async_copy(
                    r_vmem.at[layer, at], r_hbm.at[layer, at], sems.at[1, layer, c]
                )
            )
    for copy in copies:
        copy.start()
    for copy in copies:
        copy.wait()


def on_device(n, inputs, gains, decays, w_qkv, w_out, s_state, r_state):
    layers, width, _, heads, hd = w_qkv.shape
    tokens, batch, shard = inputs.shape
    parts = PARTS if batch % (8 * PARTS) == 0 else 1
    span = batch // parts
    rows = tokens * span
    mixed = 3 * heads
    pack = 2 if heads % 2 == 0 else 1
    groups = mixed // pack
    chips = n // 2
    vmem = pl.BlockSpec(memory_space=pltpu.VMEM)
    anywhere = pl.BlockSpec(memory_space=pl.ANY)
    if pack == 1:
        w_view = w_qkv.reshape(layers, width, mixed * hd)
        w_vmem = pltpu.VMEM(w_view.shape, BF16)
    else:
        w_view = w_qkv.reshape(layers, width // 8, 8, groups, pack, hd)
        w_vmem = pltpu.VMEM((layers, width // 8, groups, 8 * pack, hd), BF16)
    blocks = (layers, parts, chips, rows, shard)
    pairs = (layers, parts, heads, 2 * rows, hd)
    dma = pltpu.SemaphoreType.DMA
    y, s_new, r_new = pl.pallas_call(
        functools.partial(front_kernel, n, tokens, batch, heads, layers, parts),
        out_shape=(
            pltpu.VMEM(inputs.shape, F32),
            pltpu.VMEM(s_state.shape, F32),
            pltpu.VMEM(r_state.shape, F32),
        ),
        in_specs=[anywhere] * 7,
        out_specs=(vmem, vmem, vmem),
        scratch_shapes=[
            pltpu.VMEM(inputs.shape, BF16),
            pltpu.VMEM((layers, width), F32),
            pltpu.SMEM(decays.shape, F32),
            w_vmem,
            pltpu.VMEM((layers, heads * hd, width), BF16),
            pltpu.VMEM((128, 128 * pack * 2), BF16),
            pltpu.VMEM((layers, parts, chips, 2, rows, shard), BF16),
            pltpu.VMEM((n, pack * rows, pack * shard), BF16),
            pltpu.VMEM((parts, pack * rows, groups * hd), F32),
            pltpu.VMEM((parts, rows, 128), F32),
            pltpu.VMEM(blocks, BF16),
            pltpu.VMEM(blocks, BF16),
            pltpu.VMEM(blocks, BF16),
            pltpu.VMEM(blocks, BF16),
            pltpu.VMEM(blocks[1:], F32),
            pltpu.VMEM((parts, rows, shard), F32),
            pltpu.VMEM((heads, 2 * rows, hd), F32),
            pltpu.VMEM((heads, 2 * rows, hd), F32),
            pltpu.VMEM((heads, 2 * rows, hd), F32),
            pltpu.VMEM((parts, rows, heads * hd), BF16),
            pltpu.VMEM(pairs, F32),
            pltpu.VMEM(pairs, F32),
            dma((3,)),
            dma((layers, PIECES)),
            dma((layers,)),
            dma((2, layers, parts)),
            dma((layers, parts, 2, chips)),
            dma((layers, parts, 2, chips)),
            dma((layers, parts, chips)),
            dma((layers, parts, chips)),
            dma((layers, parts, chips)),
            dma((layers, parts, chips)),
        ],
        compiler_params=pltpu.CompilerParams(
            collective_id=0, has_side_effects=True, vmem_limit_bytes=44 * 1024 * 1024
        ),
        name="front",
    )(
        inputs,
        gains,
        decays,
        w_view,
        w_out.reshape(layers, heads * hd, width),
        s_state,
        r_state,
    )
    return pl.pallas_call(
        back_kernel,
        out_shape=tuple(
            jax.ShapeDtypeStruct(a.shape, F32) for a in (inputs, s_state, r_state)
        ),
        in_specs=[vmem] * 3,
        out_specs=(anywhere,) * 3,
        scratch_shapes=[dma((3, layers, 4))],
        compiler_params=pltpu.CompilerParams(vmem_limit_bytes=1024 * 1024),
        name="back",
    )(y, s_new, r_new)


def solution(mesh):
    in_specs = (
        P(None, "grp", "head"),
        P(),
        P(None, "head"),
        P(None, None, None, "head", None),
        P(None, "head", None, None),
        P(None, "grp", "head", None, None),
        P(None, "grp", "head", None, None),
    )
    out_specs = (
        P(None, "grp", "head"),
        P(None, "grp", "head", None, None),
        P(None, "grp", "head", None, None),
    )
    return jax.shard_map(
        functools.partial(on_device, mesh.shape["head"]),
        mesh=mesh,
        in_specs=in_specs,
        out_specs=out_specs,
        check_vma=False,
    )
```

```python
import functools

import jax
import jax.numpy as jnp
from jax import lax
from jax.experimental import pallas as pl
from jax.experimental.pallas import tpu as pltpu
from jax.sharding import PartitionSpec as P

EPSILON = 1e-05
PARTS = 2
CUTS = 4
F32 = jnp.float32
BF16 = jnp.bfloat16
MESH = pl.DeviceIdType.MESH


def front_kernel(
    n, tokens, batch, heads, layers, parts,
    x_hbm, gains_hbm, dec_hbm, w_hbm, wo_hbm, s_hbm, r_hbm,
    y_ref, sv, rv,
    xin, gains_ref, dec_ref, w, wo, spread, xg, lhs, acc, squares, near, far, pair, recv, mine, cur,
    kq, pz, os, oo, left_ref, right_ref,
    misc_sem, w_sem, wo_sem, state_sem, out_sem, ag_recv, rs_recv,
):
    me = lax.axis_index("head")
    side = lax.rem(me, 2)
    chip = me // 2
    chips = n // 2
    sibling = me + 1 - 2 * side
    hd = kq.shape[-1]
    width = gains_ref.shape[1]
    shard = xin.shape[2]
    full = tokens * batch
    rows = full // parts
    mixed = 3 * heads
    pack = lhs.shape[1] // full
    groups = mixed // pack

    def w_rows(k):
        unit = 2 * shard // (8 if pack > 1 else 1)
        at = lax.rem(chip - k + chips, chips) * unit
        return pl.ds(pl.multiple_of(at, unit), unit)

    def w_copies(layer):
        out = []
        for k in range(chips):
            at, sem = w_rows(k), w_sem.at[layer, k]
            if pack == 1:
                out.append(pltpu.make_async_copy(w_hbm.at[layer, at], w.at[layer, at], sem))
                continue
            for s in range(8):
                out.append(
                    pltpu.make_async_copy(
                        w_hbm.at[layer, at, s],
                        w.at[layer, at, :, pl.ds(s * pack, pack)],
                        sem,
                    )
                )
        return out

    def w_wait(layer, k):
        part = w.at[layer, w_rows(k)]
        pltpu.make_async_copy(part, part, w_sem.at[layer, k]).wait()

    def wo_copy(layer):
        return pltpu.make_async_copy(wo_hbm.at[layer], wo.at[layer], wo_sem.at[layer])

    def state_copy(which, layer):
        src, dst = ((r_hbm, rv), (s_hbm, sv))[which]
        return pltpu.make_async_copy(src.at[layer], dst.at[layer], state_sem.at[which, layer])

    def send(layer, kind, src, dst, in_sem, peer):
        pltpu.make_async_remote_copy(
            src_ref=src,
            dst_ref=dst,
            send_sem=out_sem.at[layer, kind],
            recv_sem=in_sem,
            device_id={"head": peer},
            device_id_type=MESH,
        ).start()

    def settle(layer):
        some = pl.ds(1, chips - 1)
        sent = (
            xg.at[layer, :, 0],
            xg.at[layer, :, 0, some],
            near.at[layer],
            pair.at[layer, :, some],
        )
        for kind, blocks in enumerate(sent):
            pltpu.make_async_copy(blocks, blocks, out_sem.at[layer, kind]).wait()

    def arrive(buf, sem):
        pltpu.make_async_copy(buf, buf, sem).wait()

    def peer(k):
        return lax.rem(me + 2 * k, n)

    def block_at(k, other):
        at = 2 * lax.rem(chip - k + chips, chips)
        return at + (1 - side if other else side)

    misc = (
        pltpu.make_async_copy(x_hbm, xin, misc_sem.at[0]),
        pltpu.make_async_copy(gains_hbm, gains_ref, misc_sem.at[1]),
        pltpu.make_async_copy(dec_hbm, dec_ref, misc_sem.at[2]),
    )
    for copy in misc:
        copy.start()
    barrier = pltpu.get_barrier_semaphore()
    for k in range(1, chips):
        pl.semaphore_signal(barrier, inc=1, device_id={"head": peer(k)}, device_id_type=MESH)
    pl.semaphore_signal(barrier, inc=1, device_id={"head": sibling}, device_id_type=MESH)
    for copy in w_copies(0):
        copy.start()
    if pack > 1:
        row = lax.broadcasted_iota(jnp.int32, spread.shape, 0)
        col = lax.broadcasted_iota(jnp.int32, spread.shape, 1)
        half = spread.shape[1] // 2
        hit = jnp.where(col < half, col - 2 * row, col - half - 2 * row - 1)
        spread[...] = jnp.where(hit == 0, 1.0, 0.0).astype(BF16)
    misc[0].wait()
    start = jnp.concatenate([xin[t] for t in range(tokens)], axis=0)
    for part in range(parts):
        rows_x = start[part * rows : (part + 1) * rows]
        cur[part] = rows_x.astype(F32)
        xg[0, part, 0, 0] = rows_x
    pl.semaphore_wait(barrier, chips)

    def gather_start(layer, part):
        own = xg.at[layer, part, 0, 0]
        for k in range(1, chips):
            send(layer, 0, own, xg.at[layer, part, 0, k], ag_recv.at[0, layer, part], peer(k))
        send(layer, 0, own, xg.at[layer, part, 1, 0], ag_recv.at[1, layer, part], sibling)

    def forward(layer, part):
        arrive(xg.at[layer, part, 0, pl.ds(1, chips - 1)], ag_recv.at[0, layer, part])
        for k in range(1, chips):
            send(
                layer, 1, xg.at[layer, part, 0, k], xg.at[layer, part, 1, k],
                ag_recv.at[2, layer, part], sibling,
            )

    def forwarded(layer, part):
        arrive(xg.at[layer, part, 1, pl.ds(1, chips - 1)], ag_recv.at[2, layer, part])

    def expand(layer, slots, which):
        stack = []
        for k, other in slots:
            i = block_at(k, other)
            gain = gains_ref[layer : layer + 1, pl.ds(pl.multiple_of(i * shard, shard), shard)]
            for part in which:
                block = xg[layer, part, other, k].astype(F32)
                square = block * block
                total = square[:, :128]
                for at in range(128, shard, 128):
                    total = total + square[:, at : at + 128]
                squares[part] = squares[part] + total
                scaled = (block * gain).astype(BF16)
                if pack == 1:
                    lhs[2 * k + other, part * rows : (part + 1) * rows] = scaled
                else:
                    stack += [scaled[:, at : at + 128] for at in range(0, shard, 128)]
        if pack == 1:
            return
        wide = spread.shape[1] // 2
        out = jnp.dot(
            jnp.concatenate(stack, axis=0), spread[...], preferred_element_type=F32
        ).astype(BF16)
        at = 0
        for k, other in slots:
            for part in which:
                for s in range(shard // 128):
                    for p in range(pack):
                        to = (p * parts + part) * rows
                        lhs[2 * k + other, to : to + rows, s * wide : (s + 1) * wide] = out[
                            at : at + rows, p * wide : (p + 1) * wide
                        ]
                    at += rows

    def multiply(layer, slots, first):
        for g in range(0, groups, 2):
            many = min(2, groups - g)
            total = None
            for k, other in slots:
                i = block_at(k, other)
                if pack == 1:
                    at = pl.ds(pl.multiple_of(i * shard, shard), shard)
                    weights = w[layer, at, g * hd : (g + many) * hd]
                else:
                    at = pl.ds(i * (shard // 8), shard // 8)
                    weights = jnp.concatenate(
                        [
                            w[layer, at, g + j].reshape(pack * shard, hd)
                            for j in range(many)
                        ],
                        axis=1,
                    )
                term = jnp.dot(lhs[2 * k + other], weights, preferred_element_type=F32)
                total = term if total is None else total + term
            cols = slice(g * hd, (g + many) * hd)
            acc[:, cols] = total if first else acc[:, cols] + total

    def project(layer):
        every, last = list(range(parts)), [parts - 1]
        home = [(0, 0), (0, 1)]
        direct = [(k, 0) for k in range(1, chips)]
        passed = [(k, 1) for k in range(1, chips)]
        squares[...] = jnp.zeros_like(squares)
        for part in every:
            arrive(xg.at[layer, part, 1, 0], ag_recv.at[1, layer, part])
        w_wait(layer, 0)
        expand(layer, home, every)
        multiply(layer, home, True)
        if layer + 1 < layers:
            for copy in w_copies(layer + 1):
                copy.start()
            for which in range(2):
                state_copy(which, layer + 1).start()
            wo_copy(layer + 1).start()
        for part in every[:-1]:
            forward(layer, part)
            expand(layer, direct, [part])
            forwarded(layer, part)
            expand(layer, passed, [part])
        forward(layer, parts - 1)
        expand(layer, direct, last)
        for k in range(1, chips):
            w_wait(layer, k)
        multiply(layer, direct, False)
        forwarded(layer, parts - 1)
        expand(layer, passed, last)
        multiply(layer, passed, False)
        total = jnp.concatenate([squares[part] for part in every], axis=0)
        return lax.rsqrt(jnp.sum(total, axis=-1, keepdims=True) / width + EPSILON)

    def norm(v):
        return v * lax.rsqrt(jnp.mean(v * v, axis=-1, keepdims=True) + EPSILON)

    def dots(a, b):
        return jnp.sum(a * b, axis=-1, keepdims=True)

    def tok(t):
        return slice(t * batch, (t + 1) * batch)

    def per_pair(fn, many):
        step = 4 if batch % 4 == 0 else 1

        def body(i, carry):
            for j in range(step):
                b = i * step + j
                for h in range(0, heads, many):
                    fn(b, list(range(h, min(h + many, heads))))
            return carry

        lax.fori_loop(0, batch // step, body, 0)

    def mesa(layer, factor):

        def projected(j, h):
            at = j * heads + h
            p, g = at % pack, at // pack
            return acc[p * full : (p + 1) * full, g * hd : (g + 1) * hd] * factor

        for h in range(heads):
            kq[h, full:, :] = norm(projected(0, h))
            kq[h, :full, :] = norm(projected(1, h)) * hd ** (-0.5)
            left_ref[layer, h, full:, :] = projected(2, h)
        state_copy(0, layer).wait()

        def first(b, hs):
            at = pl.ds(b, 2 * tokens, stride=batch)
            both = jnp.concatenate([kq[h, at, :] for h in hs], axis=0).astype(BF16)
            mats = jnp.concatenate([rv[layer, b, h].astype(BF16) for h in hs], axis=1)
            out = jnp.dot(both, mats, preferred_element_type=F32)
            for j, h in enumerate(hs):
                pz[h, at, :] = out[
                    j * 2 * tokens : (j + 1) * 2 * tokens, j * hd : (j + 1) * hd
                ]

        per_pair(first, 2)
        for h in range(heads):
            g = jnp.full((batch, 1), dec_ref[layer, h], F32)
            ginv = 1.0 / g
            ks = [kq[h, tok(t), :] for t in range(tokens)]
            qs = [kq[h, tok(tokens + t), :] for t in range(tokens)]
            ps = [pz[h, tok(t), :] for t in range(tokens)]
            zs = [pz[h, tok(tokens + t), :] for t in range(tokens)]
            back = [None] * (tokens + 1)
            front = [None] * (tokens + 1)
            back[0] = front[0] = jnp.ones_like(g)
            for t in range(tokens):
                back[t + 1] = back[t] * ginv
                front[t + 1] = front[t] * g
            for t in range(tokens):
                u = ps[t]
                inv = 1.0 / (g + dots(ks[t], u))
                for s in range(t + 1, tokens):
                    ps[s] = (ps[s] - u * (dots(u, ks[s]) * inv)) * ginv
                for s in range(t, tokens):
                    zs[s] = (zs[s] - u * (dots(u, qs[s]) * inv)) * ginv
                left_ref[layer, h, tok(t), :] = u
                right_ref[layer, h, tok(t), :] = u * (-inv * back[tokens - t])
                right_ref[layer, h, tok(tokens + t), :] = ks[t] * front[tokens - 1 - t]
                pz[h, tok(t), :] = zs[t]
        state_copy(1, layer).wait()

        def second(b, hs):
            at = pl.ds(b, 2 * tokens, stride=batch)
            both = jnp.concatenate([pz[h, at, :] for h in hs], axis=0).astype(BF16)
            mats = jnp.concatenate([sv[layer, b, h].astype(BF16) for h in hs], axis=0)
            out = lax.dot_general(
                both, mats, (((1,), (1,)), ((), ())), preferred_element_type=F32
            )
            for j, h in enumerate(hs):
                os[h, at, :] = out[
                    j * 2 * tokens : (j + 1) * 2 * tokens, j * hd : (j + 1) * hd
                ]

        per_pair(second, 2)
        for h in range(heads):
            g = jnp.full((batch, 1), dec_ref[layer, h], F32)
            front = [jnp.ones_like(g)]
            for t in range(tokens):
                front.append(front[-1] * g)
            outs = []
            for t in range(tokens):
                z = pz[h, tok(t), :]
                out = os[h, tok(t), :] * front[t + 1]
                for s in range(t + 1):
                    v = left_ref[layer, h, tok(tokens + s), :]
                    out = out + v * (dots(kq[h, tok(s), :], z) * front[t - s])
                outs.append(out)
            oo[:, h * hd : (h + 1) * hd] = jnp.concatenate(outs, axis=0).astype(BF16)

    def update(layer):
        upper = lax.broadcasted_iota(jnp.int32, (2 * tokens, hd), 0) < tokens
        scales = []
        for h in range(heads):
            g = jnp.full((1, hd), dec_ref[layer, h], F32)
            power = g
            for _ in range(tokens - 1):
                power = power * g
            scales.append((power, 1.0 / power))

        def change_of(b, hs):
            h = hs[0]
            at = pl.ds(b, 2 * tokens, stride=batch)
            left = left_ref[layer, h, at, :]
            right = right_ref[layer, h, at, :]
            zero = jnp.zeros_like(right)
            both = jnp.concatenate(
                [jnp.where(upper, right, zero), jnp.where(upper, zero, right)], axis=1
            ).astype(BF16)
            change = jnp.dot(left.T.astype(BF16), both, preferred_element_type=F32)
            rv[layer, b, h] = rv[layer, b, h] * scales[h][1] + change[:, :hd]
            sv[layer, b, h] = sv[layer, b, h] * scales[h][0] + change[:, hd:]

        per_pair(change_of, 1)

    def mix(layer):
        def product(k, other):
            i = 2 * lax.rem(chip + k, chips) + (1 - side if other else side)
            col = pl.ds(pl.multiple_of(i * shard, shard), shard)
            return jnp.dot(oo[...], wo[layer, :, col], preferred_element_type=F32)

        order = list(range(1, chips)) + [0]
        for k in order:
            out = product(k, 1).astype(BF16)
            for part in range(parts):
                near[layer, part, k] = out[part * rows : (part + 1) * rows]
        for part in range(parts):
            for k in order:
                send(
                    layer, 2, near.at[layer, part, k], far.at[layer, part, k],
                    rs_recv.at[0, layer, part], sibling,
                )
        for k in order:
            out = product(k, 0)
            for part in range(parts):
                mine[part, k] = out[part * rows : (part + 1) * rows]

    def scatter(layer, part):
        arrive(far.at[layer, part], rs_recv.at[0, layer, part])
        for k in range(1, chips):
            pair[layer, part, k] = (
                mine[part, k] + far[layer, part, k].astype(F32)
            ).astype(BF16)
            send(
                layer, 3, pair.at[layer, part, k], recv.at[layer, part, k],
                rs_recv.at[1, layer, part], peer(k),
            )

    def collect(layer, part):
        total = cur[part] + mine[part, 0] + far[layer, part, 0].astype(F32)
        arrive(recv.at[layer, part, pl.ds(1, chips - 1)], rs_recv.at[1, layer, part])
        for k in range(1, chips):
            total = total + recv[layer, part, k].astype(F32)
        cur[part] = total
        if layer + 1 < layers:
            xg[layer + 1, part, 0, 0] = total.astype(BF16)
            gather_start(layer + 1, part)
        else:
            y_ref[part * rows : (part + 1) * rows, :] = total

    every = range(parts)
    for part in every:
        gather_start(0, part)
    for copy in misc[1:]:
        copy.wait()
    state_copy(0, 0).start()
    state_copy(1, 0).start()
    wo_copy(0).start()
    for layer in range(layers):
        factor = project(layer)
        mesa(layer, factor)
        wo_copy(layer).wait()
        mix(layer)
        for part in every:
            scatter(layer, part)
        if layer + 1 < layers:
            update(layer)
            for part in every:
                collect(layer, part)
        else:
            update(layer)
            for at in range(layers - 1):
                settle(at)
            for part in every:
                collect(layer, part)
    settle(layers - 1)


def back_kernel(y_vmem, s_vmem, r_vmem, y_hbm, s_hbm, r_hbm, sems):
    whole = []
    for i, (src, dst) in enumerate(((s_vmem, s_hbm), (r_vmem, r_hbm), (y_vmem, y_hbm))):
        whole.append(pltpu.make_async_copy(src, dst, sems.at[i]))
        if i == 2:
            whole[i].start()
            continue
        cut = src.shape[1] // CUTS
        for layer in range(src.shape[0]):
            for c in range(CUTS):
                at = (layer, pl.ds(c * cut, cut))
                pltpu.make_async_copy(src.at[at], dst.at[at], sems.at[i]).start()
    for copy in whole:
        copy.wait()


def on_device(n, inputs, gains, decays, w_qkv, w_out, s_state, r_state):
    layers, width, _, heads, hd = w_qkv.shape
    tokens, batch, shard = inputs.shape
    full = tokens * batch
    parts = PARTS if full % (16 * PARTS) == 0 else 1
    rows = full // parts
    mixed = 3 * heads
    pack = 2 if heads % 2 == 0 else 1
    groups = mixed // pack
    chips = n // 2
    vmem = pl.BlockSpec(memory_space=pltpu.VMEM)
    anywhere = pl.BlockSpec(memory_space=pl.ANY)
    if pack == 1:
        w_view = w_qkv.reshape(layers, width, mixed * hd)
        w_vmem = pltpu.VMEM(w_view.shape, BF16)
    else:
        w_view = w_qkv.reshape(layers, width // 8, 8, groups, pack, hd)
        w_vmem = pltpu.VMEM((layers, width // 8, groups, 8 * pack, hd), BF16)
    blocks = (layers, parts, chips, rows, shard)
    pairs = (layers, heads, 2 * full, hd)
    dma = pltpu.SemaphoreType.DMA
    y, s_new, r_new = pl.pallas_call(
        functools.partial(front_kernel, n, tokens, batch, heads, layers, parts),
        out_shape=(
            pltpu.VMEM((full, shard), F32),
            pltpu.VMEM(s_state.shape, F32),
            pltpu.VMEM(r_state.shape, F32),
        ),
        in_specs=[anywhere] * 7,
        out_specs=(vmem, vmem, vmem),
        scratch_shapes=[
            pltpu.VMEM(inputs.shape, BF16),
            pltpu.VMEM((layers, width), F32),
            pltpu.SMEM(decays.shape, F32),
            w_vmem,
            pltpu.VMEM((layers, heads * hd, width), BF16),
            pltpu.VMEM((128, 128 * pack * 2), BF16),
            pltpu.VMEM((layers, parts, 2, chips, rows, shard), BF16),
            pltpu.VMEM((n, pack * full, pack * shard), BF16),
            pltpu.VMEM((pack * full, groups * hd), F32),
            pltpu.VMEM((parts, rows, 128), F32),
            pltpu.VMEM(blocks, BF16),
            pltpu.VMEM(blocks, BF16),
            pltpu.VMEM(blocks, BF16),
            pltpu.VMEM(blocks, BF16),
            pltpu.VMEM(blocks[1:], F32),
            pltpu.VMEM((parts, rows, shard), F32),
            pltpu.VMEM((heads, 2 * full, hd), F32),
            pltpu.VMEM((heads, 2 * full, hd), F32),
            pltpu.VMEM((heads, 2 * full, hd), F32),
            pltpu.VMEM((full, heads * hd), BF16),
            pltpu.VMEM(pairs, F32),
            pltpu.VMEM(pairs, F32),
            dma((3,)),
            dma((layers, chips)),
            dma((layers,)),
            dma((2, layers)),
            dma((layers, 4)),
            dma((3, layers, parts)),
            dma((2, layers, parts)),
        ],
        compiler_params=pltpu.CompilerParams(
            collective_id=0, has_side_effects=True, vmem_limit_bytes=44 * 1024 * 1024
        ),
        name="front",
    )(
        inputs,
        gains,
        decays,
        w_view,
        w_out.reshape(layers, heads * hd, width),
        s_state,
        r_state,
    )
    out = pl.pallas_call(
        back_kernel,
        out_shape=tuple(jax.ShapeDtypeStruct(a.shape, F32) for a in (y, s_state, r_state)),
        in_specs=[vmem] * 3,
        out_specs=(anywhere,) * 3,
        scratch_shapes=[dma((3,))],
        compiler_params=pltpu.CompilerParams(vmem_limit_bytes=1024 * 1024),
        name="back",
    )(y, s_new, r_new)
    return out[0].reshape(inputs.shape), out[1], out[2]


def solution(mesh):
    in_specs = (
        P(None, "grp", "head"),
        P(),
        P(None, "head"),
        P(None, None, None, "head", None),
        P(None, "head", None, None),
        P(None, "grp", "head", None, None),
        P(None, "grp", "head", None, None),
    )
    out_specs = (
        P(None, "grp", "head"),
        P(None, "grp", "head", None, None),
        P(None, "grp", "head", None, None),
    )
    return jax.shard_map(
        functools.partial(on_device, mesh.shape["head"]),
        mesh=mesh,
        in_specs=in_specs,
        out_specs=out_specs,
        check_vma=False,
    )
```

```python
import functools

import jax
import jax.numpy as jnp
from jax import lax
from jax.experimental import pallas as pl
from jax.experimental.pallas import tpu as pltpu
from jax.sharding import PartitionSpec as P

EPSILON = 1e-05
PARTS = 2
CUTS = 4
F32 = jnp.float32
BF16 = jnp.bfloat16
MESH = pl.DeviceIdType.MESH


def front_kernel(
    n, tokens, batch, heads, layers, parts,
    x_hbm, gains_hbm, dec_hbm, w_hbm, wo_hbm, s_hbm, r_hbm,
    y_ref, sv, rv,
    xin, gains_ref, dec_ref, w, wo, spread, xg, lhs, acc, squares, near, far, pair, recv, mine, cur,
    kq, pz, os, oo, left_ref, right_ref,
    misc_sem, w_sem, wo_sem, state_sem, out_sem, ag_recv, rs_recv,
):
    me = lax.axis_index("head")
    side = lax.rem(me, 2)
    chip = me // 2
    chips = n // 2
    sibling = me + 1 - 2 * side
    hd = kq.shape[-1]
    width = gains_ref.shape[1]
    shard = xin.shape[2]
    full = tokens * batch
    rows = full // parts
    mixed = 3 * heads
    pack = lhs.shape[1] // full
    groups = mixed // pack

    def w_rows(k):
        unit = 2 * shard // (8 if pack > 1 else 1)
        at = lax.rem(chip - k + chips, chips) * unit
        return pl.ds(pl.multiple_of(at, unit), unit)

    def w_copies(layer):
        out = []
        for k in range(chips):
            at, sem = w_rows(k), w_sem.at[layer, k]
            if pack == 1:
                out.append(pltpu.make_async_copy(w_hbm.at[layer, at], w.at[layer, at], sem))
                continue
            for s in range(8):
                out.append(
                    pltpu.make_async_copy(
                        w_hbm.at[layer, at, s],
                        w.at[layer, at, :, pl.ds(s * pack, pack)],
                        sem,
                    )
                )
        return out

    def w_wait(layer, k):
        part = w.at[layer, w_rows(k)]
        pltpu.make_async_copy(part, part, w_sem.at[layer, k]).wait()

    def wo_copy(layer):
        return pltpu.make_async_copy(wo_hbm.at[layer], wo.at[layer], wo_sem.at[layer])

    def state_copy(which, layer):
        src, dst = ((r_hbm, rv), (s_hbm, sv))[which]
        return pltpu.make_async_copy(src.at[layer], dst.at[layer], state_sem.at[which, layer])

    def send(layer, kind, src, dst, in_sem, peer):
        pltpu.make_async_remote_copy(
            src_ref=src,
            dst_ref=dst,
            send_sem=out_sem.at[layer, kind],
            recv_sem=in_sem,
            device_id={"head": peer},
            device_id_type=MESH,
        ).start()

    def settle(layer):
        some = pl.ds(1, chips - 1)
        sent = (
            xg.at[layer, :, 0],
            xg.at[layer, :, 0, some],
            near.at[layer],
            pair.at[layer, :, some],
        )
        for kind, blocks in enumerate(sent):
            pltpu.make_async_copy(blocks, blocks, out_sem.at[layer, kind]).wait()

    def arrive(buf, sem):
        pltpu.make_async_copy(buf, buf, sem).wait()

    def peer(k):
        return lax.rem(me + 2 * k, n)

    def block_at(k, other):
        at = 2 * lax.rem(chip - k + chips, chips)
        return at + (1 - side if other else side)

    misc = (
        pltpu.make_async_copy(x_hbm, xin, misc_sem.at[0]),
        pltpu.make_async_copy(gains_hbm, gains_ref, misc_sem.at[1]),
        pltpu.make_async_copy(dec_hbm, dec_ref, misc_sem.at[2]),
    )
    for copy in misc:
        copy.start()
    barrier = pltpu.get_barrier_semaphore()
    for k in range(1, chips):
        pl.semaphore_signal(barrier, inc=1, device_id={"head": peer(k)}, device_id_type=MESH)
    pl.semaphore_signal(barrier, inc=1, device_id={"head": sibling}, device_id_type=MESH)
    for copy in w_copies(0):
        copy.start()
    if pack > 1:
        row = lax.broadcasted_iota(jnp.int32, spread.shape, 0)
        col = lax.broadcasted_iota(jnp.int32, spread.shape, 1)
        half = spread.shape[1] // 2
        hit = jnp.where(col < half, col - 2 * row, col - half - 2 * row - 1)
        spread[...] = jnp.where(hit == 0, 1.0, 0.0).astype(BF16)
    misc[0].wait()
    start = jnp.concatenate([xin[t] for t in range(tokens)], axis=0)
    for part in range(parts):
        rows_x = start[part * rows : (part + 1) * rows]
        cur[part] = rows_x.astype(F32)
        xg[0, part, 0, 0] = rows_x
    pl.semaphore_wait(barrier, chips)

    def gather_start(layer, part):
        own = xg.at[layer, part, 0, 0]
        for k in range(1, chips):
            send(layer, 0, own, xg.at[layer, part, 0, k], ag_recv.at[0, layer, part], peer(k))
        send(layer, 0, own, xg.at[layer, part, 1, 0], ag_recv.at[1, layer, part], sibling)

    def forward(layer, part):
        arrive(xg.at[layer, part, 0, pl.ds(1, chips - 1)], ag_recv.at[0, layer, part])
        for k in range(1, chips):
            send(
                layer, 1, xg.at[layer, part, 0, k], xg.at[layer, part, 1, k],
                ag_recv.at[2, layer, part], sibling,
            )

    def forwarded(layer, part):
        arrive(xg.at[layer, part, 1, pl.ds(1, chips - 1)], ag_recv.at[2, layer, part])

    def expand(layer, slots, which):
        stack = []
        for k, other in slots:
            i = block_at(k, other)
            gain = gains_ref[layer : layer + 1, pl.ds(pl.multiple_of(i * shard, shard), shard)]
            for part in which:
                block = xg[layer, part, other, k].astype(F32)
                square = block * block
                total = square[:, :128]
                for at in range(128, shard, 128):
                    total = total + square[:, at : at + 128]
                squares[part] = squares[part] + total
                scaled = (block * gain).astype(BF16)
                if pack == 1:
                    lhs[2 * k + other, part * rows : (part + 1) * rows] = scaled
                else:
                    stack += [scaled[:, at : at + 128] for at in range(0, shard, 128)]
        if pack == 1:
            return
        wide = spread.shape[1] // 2
        out = jnp.dot(
            jnp.concatenate(stack, axis=0), spread[...], preferred_element_type=F32
        ).astype(BF16)
        at = 0
        for k, other in slots:
            for part in which:
                for s in range(shard // 128):
                    for p in range(pack):
                        to = (p * parts + part) * rows
                        lhs[2 * k + other, to : to + rows, s * wide : (s + 1) * wide] = out[
                            at : at + rows, p * wide : (p + 1) * wide
                        ]
                    at += rows

    def multiply(layer, slots, first):
        for g in range(0, groups, 2):
            many = min(2, groups - g)
            total = None
            for k, other in slots:
                i = block_at(k, other)
                if pack == 1:
                    at = pl.ds(pl.multiple_of(i * shard, shard), shard)
                    weights = w[layer, at, g * hd : (g + many) * hd]
                else:
                    at = pl.ds(i * (shard // 8), shard // 8)
                    weights = jnp.concatenate(
                        [
                            w[layer, at, g + j].reshape(pack * shard, hd)
                            for j in range(many)
                        ],
                        axis=1,
                    )
                term = jnp.dot(lhs[2 * k + other], weights, preferred_element_type=F32)
                total = term if total is None else total + term
            cols = slice(g * hd, (g + many) * hd)
            acc[:, cols] = total if first else acc[:, cols] + total

    def project(layer):
        every, last = list(range(parts)), [parts - 1]
        home, beside = [(0, 0)], [(0, 1)]
        direct = [(k, 0) for k in range(1, chips)]
        passed = [(k, 1) for k in range(1, chips)]
        squares[...] = jnp.zeros_like(squares)
        w_wait(layer, 0)
        expand(layer, home, every)
        multiply(layer, home, True)
        if layer + 1 < layers:
            for copy in w_copies(layer + 1):
                copy.start()
            for which in range(2):
                state_copy(which, layer + 1).start()
            wo_copy(layer + 1).start()
        for part in every[:-1]:
            forward(layer, part)
            expand(layer, direct, [part])
        for part in every:
            arrive(xg.at[layer, part, 1, 0], ag_recv.at[1, layer, part])
        expand(layer, beside, every)
        for part in every[:-1]:
            forwarded(layer, part)
            expand(layer, passed, [part])
        forward(layer, parts - 1)
        expand(layer, direct, last)
        for k in range(1, chips):
            w_wait(layer, k)
        multiply(layer, beside + direct, False)
        forwarded(layer, parts - 1)
        expand(layer, passed, last)
        multiply(layer, passed, False)
        total = jnp.concatenate([squares[part] for part in every], axis=0)
        return lax.rsqrt(jnp.sum(total, axis=-1, keepdims=True) / width + EPSILON)

    def norm(v):
        return v * lax.rsqrt(jnp.mean(v * v, axis=-1, keepdims=True) + EPSILON)

    def dots(a, b):
        return jnp.sum(a * b, axis=-1, keepdims=True)

    def tok(t):
        return slice(t * batch, (t + 1) * batch)

    def per_pair(fn, many):
        step = 4 * many if batch % (4 * many) == 0 else 1

        def body(i, carry):
            for j in range(step):
                b = i * step + j
                for h in range(0, heads, many):
                    fn(b, list(range(h, min(h + many, heads))))
            return carry

        lax.fori_loop(0, batch // step, body, 0)

    def mesa(layer, factor):

        def projected(j, h):
            at = j * heads + h
            p, g = at % pack, at // pack
            return acc[p * full : (p + 1) * full, g * hd : (g + 1) * hd] * factor

        for h in range(heads):
            kq[h, full:, :] = norm(projected(0, h))
            kq[h, :full, :] = norm(projected(1, h)) * hd ** (-0.5)
            left_ref[layer, h, full:, :] = projected(2, h)
        state_copy(0, layer).wait()

        def first(b, hs):
            at = pl.ds(b, 2 * tokens, stride=batch)
            both = jnp.concatenate([kq[h, at, :] for h in hs], axis=0).astype(BF16)
            mats = jnp.concatenate([rv[layer, b, h].astype(BF16) for h in hs], axis=1)
            out = jnp.dot(both, mats, preferred_element_type=F32)
            for j, h in enumerate(hs):
                pz[h, at, :] = out[
                    j * 2 * tokens : (j + 1) * 2 * tokens, j * hd : (j + 1) * hd
                ]

        per_pair(first, 2)
        for h in range(heads):
            g = jnp.full((batch, 1), dec_ref[layer, h], F32)
            ginv = 1.0 / g
            ks = [kq[h, tok(t), :] for t in range(tokens)]
            qs = [kq[h, tok(tokens + t), :] for t in range(tokens)]
            ps = [pz[h, tok(t), :] for t in range(tokens)]
            zs = [pz[h, tok(tokens + t), :] for t in range(tokens)]
            back = [None] * (tokens + 1)
            front = [None] * (tokens + 1)
            back[0] = front[0] = jnp.ones_like(g)
            for t in range(tokens):
                back[t + 1] = back[t] * ginv
                front[t + 1] = front[t] * g
            for t in range(tokens):
                u = ps[t]
                inv = 1.0 / (g + dots(ks[t], u))
                for s in range(t + 1, tokens):
                    ps[s] = (ps[s] - u * (dots(u, ks[s]) * inv)) * ginv
                for s in range(t, tokens):
                    zs[s] = (zs[s] - u * (dots(u, qs[s]) * inv)) * ginv
                left_ref[layer, h, tok(t), :] = u
                right_ref[layer, h, tok(t), :] = u * (-inv * back[tokens - t])
                right_ref[layer, h, tok(tokens + t), :] = ks[t] * front[tokens - 1 - t]
                pz[h, tok(t), :] = zs[t]
        state_copy(1, layer).wait()

        def second(b, hs):
            at = pl.ds(b, 2 * tokens, stride=batch)
            both = jnp.concatenate([pz[h, at, :] for h in hs], axis=0).astype(BF16)
            mats = jnp.concatenate([sv[layer, b, h].astype(BF16) for h in hs], axis=0)
            out = lax.dot_general(
                both, mats, (((1,), (1,)), ((), ())), preferred_element_type=F32
            )
            for j, h in enumerate(hs):
                os[h, at, :] = out[
                    j * 2 * tokens : (j + 1) * 2 * tokens, j * hd : (j + 1) * hd
                ]

        per_pair(second, 2)
        for h in range(heads):
            g = jnp.full((batch, 1), dec_ref[layer, h], F32)
            front = [jnp.ones_like(g)]
            for t in range(tokens):
                front.append(front[-1] * g)
            outs = []
            for t in range(tokens):
                z = pz[h, tok(t), :]
                out = os[h, tok(t), :] * front[t + 1]
                for s in range(t + 1):
                    v = left_ref[layer, h, tok(tokens + s), :]
                    out = out + v * (dots(kq[h, tok(s), :], z) * front[t - s])
                outs.append(out)
            oo[:, h * hd : (h + 1) * hd] = jnp.concatenate(outs, axis=0).astype(BF16)

    def update(layer):
        upper = lax.broadcasted_iota(jnp.int32, (2 * tokens, hd), 0) < tokens
        scales = []
        for h in range(heads):
            g = jnp.full((1, hd), dec_ref[layer, h], F32)
            power = g
            for _ in range(tokens - 1):
                power = power * g
            scales.append((power, 1.0 / power))

        def change_of(b, hs):
            h = hs[0]
            at = pl.ds(b, 2 * tokens, stride=batch)
            left = left_ref[layer, h, at, :]
            right = right_ref[layer, h, at, :]
            zero = jnp.zeros_like(right)
            both = jnp.concatenate(
                [jnp.where(upper, right, zero), jnp.where(upper, zero, right)], axis=1
            ).astype(BF16)
            change = jnp.dot(left.T.astype(BF16), both, preferred_element_type=F32)
            rv[layer, b, h] = rv[layer, b, h] * scales[h][1] + change[:, :hd]
            sv[layer, b, h] = sv[layer, b, h] * scales[h][0] + change[:, hd:]

        per_pair(change_of, 1)

    def mix(layer):
        def product(k, other):
            i = 2 * lax.rem(chip + k, chips) + (1 - side if other else side)
            col = pl.ds(pl.multiple_of(i * shard, shard), shard)
            return jnp.dot(oo[...], wo[layer, :, col], preferred_element_type=F32)

        order = list(range(1, chips)) + [0]
        for k in order:
            out = product(k, 1).astype(BF16)
            for part in range(parts):
                near[layer, part, k] = out[part * rows : (part + 1) * rows]
        for part in range(parts):
            for k in order:
                send(
                    layer, 2, near.at[layer, part, k], far.at[layer, part, k],
                    rs_recv.at[0, layer, part], sibling,
                )
        for k in order:
            out = product(k, 0)
            for part in range(parts):
                mine[part, k] = out[part * rows : (part + 1) * rows]

    def scatter(layer, part):
        arrive(far.at[layer, part], rs_recv.at[0, layer, part])
        for k in range(1, chips):
            pair[layer, part, k] = (
                mine[part, k] + far[layer, part, k].astype(F32)
            ).astype(BF16)
            send(
                layer, 3, pair.at[layer, part, k], recv.at[layer, part, k],
                rs_recv.at[1, layer, part], peer(k),
            )

    def collect(layer, part):
        total = cur[part] + mine[part, 0] + far[layer, part, 0].astype(F32)
        arrive(recv.at[layer, part, pl.ds(1, chips - 1)], rs_recv.at[1, layer, part])
        for k in range(1, chips):
            total = total + recv[layer, part, k].astype(F32)
        cur[part] = total
        if layer + 1 < layers:
            xg[layer + 1, part, 0, 0] = total.astype(BF16)
            gather_start(layer + 1, part)
        else:
            y_ref[part * rows : (part + 1) * rows, :] = total

    every = range(parts)
    for part in every:
        gather_start(0, part)
    for copy in misc[1:]:
        copy.wait()
    state_copy(0, 0).start()
    state_copy(1, 0).start()
    wo_copy(0).start()
    for layer in range(layers):
        factor = project(layer)
        mesa(layer, factor)
        wo_copy(layer).wait()
        mix(layer)
        for part in every:
            scatter(layer, part)
        if layer + 1 < layers:
            update(layer)
            for part in every:
                collect(layer, part)
        else:
            update(layer)
            for at in range(layers - 1):
                settle(at)
            for part in every:
                collect(layer, part)
    settle(layers - 1)


def back_kernel(y_vmem, s_vmem, r_vmem, y_hbm, s_hbm, r_hbm, sems):
    whole = []
    for i, (src, dst) in enumerate(((s_vmem, s_hbm), (r_vmem, r_hbm), (y_vmem, y_hbm))):
        whole.append(pltpu.make_async_copy(src, dst, sems.at[i]))
        if i == 2:
            whole[i].start()
            continue
        cut = src.shape[1] // CUTS
        for layer in range(src.shape[0]):
            for c in range(CUTS):
                at = (layer, pl.ds(c * cut, cut))
                pltpu.make_async_copy(src.at[at], dst.at[at], sems.at[i]).start()
    for copy in whole:
        copy.wait()


def on_device(n, inputs, gains, decays, w_qkv, w_out, s_state, r_state):
    layers, width, _, heads, hd = w_qkv.shape
    tokens, batch, shard = inputs.shape
    full = tokens * batch
    parts = PARTS if full % (16 * PARTS) == 0 else 1
    rows = full // parts
    mixed = 3 * heads
    pack = 2 if heads % 2 == 0 else 1
    groups = mixed // pack
    chips = n // 2
    vmem = pl.BlockSpec(memory_space=pltpu.VMEM)
    anywhere = pl.BlockSpec(memory_space=pl.ANY)
    if pack == 1:
        w_view = w_qkv.reshape(layers, width, mixed * hd)
        w_vmem = pltpu.VMEM(w_view.shape, BF16)
    else:
        w_view = w_qkv.reshape(layers, width // 8, 8, groups, pack, hd)
        w_vmem = pltpu.VMEM((layers, width // 8, groups, 8 * pack, hd), BF16)
    blocks = (layers, parts, chips, rows, shard)
    pairs = (layers, heads, 2 * full, hd)
    dma = pltpu.SemaphoreType.DMA
    y, s_new, r_new = pl.pallas_call(
        functools.partial(front_kernel, n, tokens, batch, heads, layers, parts),
        out_shape=(
            pltpu.VMEM((full, shard), F32),
            pltpu.VMEM(s_state.shape, F32),
            pltpu.VMEM(r_state.shape, F32),
        ),
        in_specs=[anywhere] * 7,
        out_specs=(vmem, vmem, vmem),
        scratch_shapes=[
            pltpu.VMEM(inputs.shape, BF16),
            pltpu.VMEM((layers, width), F32),
            pltpu.SMEM(decays.shape, F32),
            w_vmem,
            pltpu.VMEM((layers, heads * hd, width), BF16),
            pltpu.VMEM((128, 128 * pack * 2), BF16),
            pltpu.VMEM((layers, parts, 2, chips, rows, shard), BF16),
            pltpu.VMEM((n, pack * full, pack * shard), BF16),
            pltpu.VMEM((pack * full, groups * hd), F32),
            pltpu.VMEM((parts, rows, 128), F32),
            pltpu.VMEM(blocks, BF16),
            pltpu.VMEM(blocks, BF16),
            pltpu.VMEM(blocks, BF16),
            pltpu.VMEM(blocks, BF16),
            pltpu.VMEM(blocks[1:], F32),
            pltpu.VMEM((parts, rows, shard), F32),
            pltpu.VMEM((heads, 2 * full, hd), F32),
            pltpu.VMEM((heads, 2 * full, hd), F32),
            pltpu.VMEM((heads, 2 * full, hd), F32),
            pltpu.VMEM((full, heads * hd), BF16),
            pltpu.VMEM(pairs, F32),
            pltpu.VMEM(pairs, F32),
            dma((3,)),
            dma((layers, chips)),
            dma((layers,)),
            dma((2, layers)),
            dma((layers, 4)),
            dma((3, layers, parts)),
            dma((2, layers, parts)),
        ],
        compiler_params=pltpu.CompilerParams(
            collective_id=0, has_side_effects=True, vmem_limit_bytes=44 * 1024 * 1024
        ),
        name="front",
    )(
        inputs,
        gains,
        decays,
        w_view,
        w_out.reshape(layers, heads * hd, width),
        s_state,
        r_state,
    )
    out = pl.pallas_call(
        back_kernel,
        out_shape=tuple(jax.ShapeDtypeStruct(a.shape, F32) for a in (y, s_state, r_state)),
        in_specs=[vmem] * 3,
        out_specs=(anywhere,) * 3,
        scratch_shapes=[dma((3,))],
        compiler_params=pltpu.CompilerParams(vmem_limit_bytes=1024 * 1024),
        name="back",
    )(y, s_new, r_new)
    return out[0].reshape(inputs.shape), out[1], out[2]


def solution(mesh):
    in_specs = (
        P(None, "grp", "head"),
        P(),
        P(None, "head"),
        P(None, None, None, "head", None),
        P(None, "head", None, None),
        P(None, "grp", "head", None, None),
        P(None, "grp", "head", None, None),
    )
    out_specs = (
        P(None, "grp", "head"),
        P(None, "grp", "head", None, None),
        P(None, "grp", "head", None, None),
    )
    return jax.shard_map(
        functools.partial(on_device, mesh.shape["head"]),
        mesh=mesh,
        in_specs=in_specs,
        out_specs=out_specs,
        check_vma=False,
    )
```
